512 devices in a mesh: pts: 128 (over z, x, core), grp: 4 (over y).
Axes of the slice: x: 4, y: 4, z: 16, core: 2. Of those that a mesh axis runs over, the one named last changes fastest.
Arguments:
- vertex_features: bfloat16 [262144, 256], P(('pts', 'grp')), may hold values from -6 to 6
- result_cotangent: bfloat16 [262144, 256], P(('pts', 'grp')), may hold values from -6 to 6
- entry_matrix: bfloat16 [256, 256], replicated, may hold values from -0.375 to 0.375
- exit_matrix: bfloat16 [256, 256], replicated, may hold values from -0.375 to 0.375
- cluster_matrix: bfloat16 [32, 64], replicated, may hold values from -4 to 4
- softmax_sharpness: float32 [8], replicated, may hold values from 0.1 to 2
- cluster_attention_matrices: float32 [3, 32, 32], replicated, may hold values from -2 to 2
- occupied_tally: int32 [512], replicated, may hold values from 170 to 512, as said below
Outputs:
- x_grad: bfloat16 [262144, 256], P(('pts', 'grp'))
- weight_grads: float32 [2, 256, 256], P(None, 'grp')
- slice_grad: float32 [32, 64], replicated
- temp_grad: float32 [8], replicated
- token_grads: float32 [3, 32, 32], replicated
The draws below stay inside these ranges and needn't reach their ends.
Inputs may be any that keep to these rules, and one draw needn't show every extreme that they name: occupied_tally[i] is the number of valid points of the i-th block of 512 point slots; they come first in the block. Some block is full and some holds 170 in every draw.
All inputs are finite; a program needn't handle non-finite values.
Results may differ from the reference program's by a relative error of at most 0.012.
The reference program's roundings to bfloat16 on the way count: a program that leaves them out, or rounds other values in their place, can miss the bound.
Values may be sent and summed in bfloat16 or wider, within the bound.
A program may use at most 64 MiB of HBM per device.

```python
import jax
import jax.numpy as jnp
from jax import lax

D = 256
H = 8
M = 64
PTS_DEV = 512
DH = 32
SHARDS = 512
POINTS = 262144


def draw_softmax_sharpness(key, part):
    base_key = jax.random.fold_in(key, 11)
    first_key, second_key, third_key = jax.random.split(base_key, 3)
    drawn_temp = jnp.exp(jax.random.uniform(first_key, (H,), jnp.float32, jnp.log(0.3), jnp.log(2.0)))
    order = jax.random.permutation(third_key, H)
    sharp = jnp.exp(jax.random.uniform(second_key, (H,), jnp.float32, jnp.log(0.15), jnp.log(0.3)))
    chosen = order < 1
    return jnp.where(chosen, sharp, drawn_temp).astype(jnp.float32)


def draw_cluster_matrix(key, part):
    base_key = jax.random.fold_in(key, 37)
    first_key, second_key = jax.random.split(base_key)
    column_scale = jnp.exp(jax.random.uniform(first_key, (1, M), jnp.float32, jnp.log(0.2), jnp.log(2.0)))
    entries = jax.random.truncated_normal(second_key, -4.0, 4.0, (DH, M), jnp.float32)
    return (entries * column_scale * (2.0 / DH) ** 0.5).astype(jnp.bfloat16)


def draw_occupied_tally(key, part):
    base_key = jax.random.fold_in(key, 23)
    first_key, second_key = jax.random.split(base_key)
    lowest = PTS_DEV // 3
    value_rows = jax.random.randint(first_key, (SHARDS,), lowest, PTS_DEV + 1, jnp.int32)
    order = jax.random.permutation(second_key, SHARDS)
    value_rows = jnp.where(order == 0, PTS_DEV, value_rows)
    value_rows = jnp.where(order == 1, lowest, value_rows)
    return value_rows.astype(jnp.int32)


def shard_levels(stream_key, dims, pieces, least, top_value):
    loudness, own = 1.0, jax.random.fold_in(stream_key, 6)
    for position, blocks in pieces:
        draws = jnp.exp(jax.random.uniform(jax.random.fold_in(own, position), (blocks,), jnp.float32, least / len(pieces), top_value / len(pieces)))
        loudness = loudness * jnp.repeat(draws, dims[position] // blocks).reshape([-1 if axis == position else 1 for axis in range(len(dims))])
    return loudness


def normal_values(rng, shape, deviation, reach, cuts=(), kind=jnp.bfloat16):
    result = jax.random.normal(rng, shape, jnp.float32) * deviation
    if len(cuts) > 0:
        result = shard_levels(rng, shape, cuts, -0.22, 0.18) * result
    return jnp.clip(result, min=-reach, max=reach).astype(kind)


def setup_inputs(seed: int = 0) -> dict:
    seeds = jax.random.split(jax.random.key(seed), 9)
    return {
        "vertex_features": normal_values(seeds[0], (POINTS, D), 1.0, 6.0, ((0, 512),)),
        "result_cotangent": normal_values(seeds[1], (POINTS, D), 1.0, 6.0, ((0, 512),)),
        "entry_matrix": normal_values(seeds[2], (D, D), D ** -0.5, 0.375),
        "exit_matrix": normal_values(seeds[3], (D, D), D ** -0.5, 0.375),
        "cluster_matrix": draw_cluster_matrix(jax.random.fold_in(seeds[8], 71), 0),
        "softmax_sharpness": draw_softmax_sharpness(jax.random.fold_in(seeds[8], 71), 0),
        "cluster_attention_matrices": normal_values(seeds[6], (3, DH, DH), (DH // 4) ** -0.5, 2.0, (), jnp.float32),
        "occupied_tally": draw_occupied_tally(jax.random.fold_in(seeds[8], 71), 0),
    }


def quantized_entries(value):
    return lax.optimization_barrier(value.astype(jnp.bfloat16)).astype(jnp.float32)


def segment_forward_sweep(feature_segment, result_cotangent_segment, validity_flags, entry_matrix, exit_matrix, cluster_matrix, softmax_sharpness):
    highest_precision = lax.Precision.HIGHEST
    point_rows = feature_segment.shape[0]
    attention_channels = softmax_sharpness.shape[0]
    single_features = quantized_entries(jnp.dot(feature_segment, entry_matrix, preferred_element_type=jnp.float32)).reshape(point_rows, attention_channels, -1)
    unscaled_product = jnp.einsum("phd,dm->phm", single_features, cluster_matrix.astype(jnp.float32), precision=highest_precision)
    cluster_scores = unscaled_product / softmax_sharpness[None, :, None]
    cluster_likelihood = jax.nn.softmax(cluster_scores, axis=-1)
    matrix_sequence = quantized_entries(cluster_likelihood * validity_flags[:, None, None])
    exit_cotangent = quantized_entries(jnp.dot(result_cotangent_segment, exit_matrix.T, preferred_element_type=jnp.float32)).reshape(point_rows, attention_channels, -1)
    return single_features, cluster_scores, cluster_likelihood, matrix_sequence, exit_cotangent


def segment_running_sums(feature_segment, result_cotangent_segment, validity_flags, entry_matrix, exit_matrix, cluster_matrix, softmax_sharpness):
    highest_precision = lax.Precision.HIGHEST
    single_features, cluster_scores, cluster_likelihood, matrix_sequence, exit_cotangent = segment_forward_sweep(feature_segment, result_cotangent_segment, validity_flags, entry_matrix, exit_matrix, cluster_matrix, softmax_sharpness)
    cluster_dividend = jnp.einsum("fzs,fzb->zsb", matrix_sequence, single_features, precision=highest_precision)
    cluster_normalizer = jnp.sum(matrix_sequence, axis=0)
    blended_cotangent = jnp.einsum("fzs,fzb->zsb", matrix_sequence, exit_cotangent, precision=highest_precision)
    return cluster_dividend, cluster_normalizer, blended_cotangent


def slice_middle(cluster_dividend, cluster_normalizer, blended_cotangent, cluster_attention_matrices):
    highest_precision = lax.Precision.HIGHEST
    clip = jnp.maximum(cluster_normalizer, 1.0)
    slice_tokens = cluster_dividend / clip[..., None]
    scale = slice_tokens.shape[-1] ** -0.5
    query_rows = jnp.einsum("cui,it->cut", slice_tokens, cluster_attention_matrices[0], precision=highest_precision)
    key_rows = jnp.einsum("cui,it->cut", slice_tokens, cluster_attention_matrices[1], precision=highest_precision)
    value_rows = jnp.einsum("cui,it->cut", slice_tokens, cluster_attention_matrices[2], precision=highest_precision)
    scores = jnp.einsum("hme,hne->hmn", query_rows, key_rows, precision=highest_precision) * scale
    attn = jax.nn.softmax(scores, axis=-1)
    mixed = jnp.einsum("hmn,hne->hme", attn, value_rows, precision=highest_precision)
    value_gradient = jnp.einsum("hmn,hme->hne", attn, blended_cotangent, precision=highest_precision)
    g_attn = jnp.einsum("hme,hne->hmn", blended_cotangent, value_rows, precision=highest_precision)
    g_scores = attn * (g_attn - jnp.sum(g_attn * attn, axis=-1, keepdims=True)) * scale
    query_gradient = jnp.einsum("hmn,hne->hme", g_scores, key_rows, precision=highest_precision)
    key_gradient = jnp.einsum("hmn,hme->hne", g_scores, query_rows, precision=highest_precision)
    query_map_gradient = jnp.einsum("sul,suv->lv", slice_tokens, query_gradient, precision=highest_precision)
    key_map_gradient = jnp.einsum("sul,suv->lv", slice_tokens, key_gradient, precision=highest_precision)
    value_map_gradient = jnp.einsum("sul,suv->lv", slice_tokens, value_gradient, precision=highest_precision)
    token_gradient = jnp.einsum("cqr,jr->cqj", query_gradient, cluster_attention_matrices[0], precision=highest_precision)
    token_gradient = token_gradient + jnp.einsum("cqr,jr->cqj", key_gradient, cluster_attention_matrices[1], precision=highest_precision)
    token_gradient = token_gradient + jnp.einsum("cqr,jr->cqj", value_gradient, cluster_attention_matrices[2], precision=highest_precision)
    g_num = token_gradient / clip[..., None]
    normalizer_cotangent = jnp.where(cluster_normalizer > 1.0, -jnp.sum(token_gradient * slice_tokens, axis=-1) / clip, 0.0)
    return mixed, g_num, normalizer_cotangent, jnp.stack([query_map_gradient, key_map_gradient, value_map_gradient])


def segment_backward_sweep(feature_segment, result_cotangent_segment, validity_flags, entry_matrix, exit_matrix, cluster_matrix, softmax_sharpness, blended_bottom_share, dividend_bottom_share, normalizer_cotangent):
    highest_precision = lax.Precision.HIGHEST
    point_rows = feature_segment.shape[0]
    single_features, cluster_scores, cluster_likelihood, matrix_sequence, exit_cotangent = segment_forward_sweep(feature_segment, result_cotangent_segment, validity_flags, entry_matrix, exit_matrix, cluster_matrix, softmax_sharpness)
    slice_weight = cluster_matrix.astype(jnp.float32)
    merged_heads = jnp.einsum("ibr,brw->ibw", matrix_sequence, blended_bottom_share, precision=highest_precision).reshape(point_rows, -1).astype(jnp.bfloat16)
    exit_matrix_cotangent = jnp.dot(merged_heads.T, result_cotangent_segment, preferred_element_type=jnp.float32)
    assign_weight_gradient = jnp.einsum("yos,ois->yoi", exit_cotangent, blended_bottom_share, precision=highest_precision)
    assign_weight_gradient = assign_weight_gradient + jnp.einsum("yos,ois->yoi", single_features, dividend_bottom_share, precision=highest_precision) + normalizer_cotangent[None]
    assign_weight_gradient = assign_weight_gradient * validity_flags[:, None, None]
    score_cotangent = cluster_likelihood * (assign_weight_gradient - jnp.sum(assign_weight_gradient * cluster_likelihood, axis=-1, keepdims=True))
    unscaled_cotangent = quantized_entries(score_cotangent / softmax_sharpness[None, :, None])
    float_input_gradient = jnp.einsum("ibr,brw->ibw", matrix_sequence, dividend_bottom_share, precision=highest_precision)
    float_input_gradient = float_input_gradient + jnp.einsum("phm,dm->phd", unscaled_cotangent, slice_weight, precision=highest_precision)
    cluster_matrix_cotangent = jnp.einsum("phd,phm->dm", single_features, unscaled_cotangent, precision=highest_precision)
    sharpness_cotangent = -jnp.sum(score_cotangent * cluster_scores, axis=(0, 2)) / softmax_sharpness
    g_xm = float_input_gradient.reshape(point_rows, -1).astype(jnp.bfloat16)
    feature_cotangent = jnp.dot(g_xm, entry_matrix.T, preferred_element_type=jnp.float32).astype(jnp.bfloat16)
    entry_matrix_cotangent = jnp.dot(feature_segment.T, g_xm, preferred_element_type=jnp.float32)
    return feature_cotangent, jnp.stack([entry_matrix_cotangent, exit_matrix_cotangent]), cluster_matrix_cotangent, sharpness_cotangent


def reference(vertex_features, result_cotangent, entry_matrix, exit_matrix, cluster_matrix, softmax_sharpness, cluster_attention_matrices, occupied_tally):
    shards = occupied_tally.shape[0]
    point_rows = vertex_features.shape[0] // shards
    width = vertex_features.shape[1]
    attention_channels = softmax_sharpness.shape[0]
    head = width // attention_channels
    slices = cluster_matrix.shape[1]
    blocks_x = vertex_features.reshape(shards, point_rows, width)
    blocks_dy = result_cotangent.reshape(shards, point_rows, width)
    live_all = (jnp.arange(point_rows, dtype=jnp.int32)[None, :] < occupied_tally[:, None]).astype(jnp.float32)

    def first(loop_state, item):
        feature_segment, result_cotangent_segment, validity_flags = item
        cluster_dividend, cluster_normalizer, blended_cotangent = segment_running_sums(feature_segment, result_cotangent_segment, validity_flags, entry_matrix, exit_matrix, cluster_matrix, softmax_sharpness)
        return (loop_state[0] + cluster_dividend, loop_state[1] + cluster_normalizer, loop_state[2] + blended_cotangent), None

    start = (jnp.zeros((attention_channels, slices, head), jnp.float32), jnp.zeros((attention_channels, slices), jnp.float32),
             jnp.zeros((attention_channels, slices, head), jnp.float32))
    totals, unused = lax.scan(first, start, (blocks_x, blocks_dy, live_all))
    mixed, g_num, normalizer_cotangent, token_grads = slice_middle(totals[0], totals[1], totals[2], cluster_attention_matrices)
    blended_bottom_share = quantized_entries(mixed)
    dividend_bottom_share = quantized_entries(g_num)

    def second(loop_state, item):
        feature_segment, result_cotangent_segment, validity_flags = item
        feature_cotangent, cotangent_sequence, cluster_matrix_cotangent, sharpness_cotangent = segment_backward_sweep(feature_segment, result_cotangent_segment, validity_flags, entry_matrix, exit_matrix, cluster_matrix, softmax_sharpness,
                                                           blended_bottom_share, dividend_bottom_share, normalizer_cotangent)
        return (loop_state[0] + cotangent_sequence, loop_state[1] + cluster_matrix_cotangent, loop_state[2] + sharpness_cotangent), feature_cotangent

    start2 = (jnp.zeros((2, width, width), jnp.float32), jnp.zeros((head, slices), jnp.float32),
              jnp.zeros((attention_channels,), jnp.float32))
    sums, x_grads = lax.scan(second, start2, (blocks_x, blocks_dy, live_all))
    x_grad = x_grads.reshape(shards * point_rows, width)
    return x_grad, sums[0], sums[1], sums[2], token_grads
```

```python
import functools

import jax
import jax.numpy as jnp
from jax import lax
from jax.experimental import pallas as pl
from jax.experimental.pallas import tpu as pltpu
from jax.sharding import Mesh
from jax.sharding import PartitionSpec as P

SIDE, GRP = 8, 4
PLANE = SIDE * GRP
HEADS, SLICES, HEAD, WIDTH = 8, 64, 32, 256
PAIRS = HEADS // 2
F32, BF16 = jnp.float32, jnp.bfloat16
EXACT = lax.Precision.HIGHEST


def dot(a, b, ca=1, cb=0, precision=None):
    return lax.dot_general(
        a, b, (((ca,), (cb,)), ((), ())), preferred_element_type=F32, precision=precision
    )


def kernel(
    depth,
    x_ref,
    y_ref,
    w_ref,
    e_ref,
    c_ref,
    t_ref,
    a_ref,
    tally_ref,
    dx_ref,
    dw_ref,
    ds_ref,
    dt_ref,
    da_ref,
    xmt,
    got,
    prob,
    logit,
    wgt,
    mrg,
    gxm,
    xt,
    tok_out,
    den_out,
    tok_in,
    den_in,
    tok_part,
    den_part,
    tok_z,
    den_z,
    tok_sum,
    den_sum,
    tok_all,
    den_all,
    g_out,
    g_in,
    s_out,
    s_in,
    g_part,
    s_part,
    g_z,
    s_z,
    g_sum,
    s_sum,
    g_all,
    s_all,
    send_sem,
    recv_sem,
):
    z, s, y = lax.axis_index("z"), lax.axis_index("s"), lax.axis_index("y")
    me = s * GRP + y
    points = x_ref.shape[0]

    def plane_peer(r):
        other = lax.rem(me + r, PLANE)
        return other, (z, other // GRP, lax.rem(other, GRP))

    def depth_peer(r):
        return (lax.rem(z + r, depth), s, y)

    def side_peer(r):
        return (z, lax.rem(s + r, SIDE), y)

    barrier = pltpu.get_barrier_semaphore()

    def greet_plane(r, carry):
        pl.semaphore_signal(
            barrier, inc=1, device_id=plane_peer(r)[1], device_id_type=pl.DeviceIdType.MESH
        )
        return carry

    def greet_depth(r, carry):
        pl.semaphore_signal(
            barrier, inc=1, device_id=depth_peer(r), device_id_type=pl.DeviceIdType.MESH
        )
        return carry

    lax.fori_loop(1, PLANE, greet_plane, 0)
    lax.fori_loop(1, depth, greet_depth, 0)

    def push(src, dst, lane, peer):
        pltpu.make_async_remote_copy(
            src_ref=src,
            dst_ref=dst,
            send_sem=send_sem.at[lane],
            recv_sem=recv_sem.at[lane],
            device_id=peer,
            device_id_type=pl.DeviceIdType.MESH,
        ).start()

    def landed(ref, lane):
        pltpu.make_async_copy(ref, ref, recv_sem.at[lane]).wait()

    def left(ref, lane):
        pltpu.make_async_copy(ref, ref, send_sem.at[lane]).wait()

    live = (
        lax.broadcasted_iota(jnp.int32, (1, points), 1) < tally_ref[z * PLANE + me]
    ).astype(F32)
    xm_all = dot(w_ref[...], x_ref[...], 0, 1).astype(BF16)
    xmt[...] = xm_all
    go_all = dot(e_ref[...], y_ref[...], 1, 1).astype(BF16)
    got[...] = go_all
    cluster = c_ref[...]
    cluster_t = cluster.astype(F32).T.astype(BF16)
    half = lax.broadcasted_iota(jnp.int32, (1, 2 * SLICES), 1) < SLICES
    ones = jnp.ones((2 * 8, points), BF16)
    rates = []
    for pair in range(PAIRS):
        for h in (2 * pair, 2 * pair + 1):
            rate = 1.0 / jnp.full((1, points), t_ref[h], F32)
            rates.append(rate)
            xm = xm_all[h * HEAD : (h + 1) * HEAD]
            raw = dot(cluster_t, xm) * rate
            e = jnp.exp(raw - jnp.max(raw, axis=0, keepdims=True))
            p = e * (1.0 / jnp.sum(e, axis=0, keepdims=True))
            rows = pl.ds(h * SLICES, SLICES)
            logit[rows, :] = raw
            prob[rows, :] = p
            wgt[rows, :] = (p * live).astype(BF16)
        w2 = wgt[pl.ds(pair * 2 * SLICES, 2 * SLICES), :]
        parts = []
        for h in (2 * pair, 2 * pair + 1):
            rows = slice(h * HEAD, (h + 1) * HEAD)
            parts.append(dot(jnp.concatenate([xm_all[rows], go_all[rows], ones]), w2, 1, 1))
        both = jnp.where(half, parts[0], parts[1])
        tok_out[pl.ds(pair * 8, 8)] = both[: 2 * HEAD].reshape(8, 8, 2 * SLICES)
        den_out[pl.ds(pair * 8, 8)] = both[2 * HEAD : 2 * HEAD + 8].reshape(8, 1, 2 * SLICES)

    pl.semaphore_wait(barrier, PLANE - 1 + depth - 1)

    def scatter_tokens(r, carry):
        other, peer = plane_peer(r)
        push(tok_out.at[other], tok_in.at[r], 0, peer)
        push(den_out.at[other], den_in.at[r], 1, peer)
        return carry

    lax.fori_loop(1, PLANE, scatter_tokens, 0)
    tok_in[0] = tok_out[me]
    den_in[0] = den_out[me]
    xt[...] = x_ref[...].T
    landed(tok_in.at[pl.ds(1, PLANE - 1)], 0)
    landed(den_in.at[pl.ds(1, PLANE - 1)], 1)
    tok_part[...] = jnp.sum(tok_in[...], axis=0)
    den_part[...] = jnp.sum(den_in[...], axis=0)

    def swap_tokens(r, carry):
        push(tok_part, tok_z.at[z], 2, depth_peer(r))
        push(den_part, den_z.at[z], 3, depth_peer(r))
        return carry

    lax.fori_loop(1, depth, swap_tokens, 0)
    tok_z[z] = tok_part[...]
    den_z[z] = den_part[...]
    landed(tok_z.at[pl.ds(0, depth - 1)], 2)
    landed(den_z.at[pl.ds(0, depth - 1)], 3)
    tok_sum[...] = jnp.sum(tok_z[...], axis=0)
    den_sum[...] = jnp.sum(den_z[...], axis=0)

    def spread_tokens(r, carry):
        peer = plane_peer(r)[1]
        push(tok_sum, tok_all.at[me], 4, peer)
        push(den_sum, den_all.at[me], 5, peer)
        return carry

    lax.fori_loop(1, PLANE, spread_tokens, 0)
    tok_all[me] = tok_sum[...]
    den_all[me] = den_sum[...]
    landed(tok_all.at[pl.ds(1, PLANE - 1)], 4)
    landed(den_all.at[pl.ds(1, PLANE - 1)], 5)

    tok4 = tok_all[...].reshape(PAIRS, 2 * HEAD, 2 * SLICES)
    num = jnp.concatenate([tok4[i, :HEAD] for i in range(PAIRS)], axis=1)
    g_mix = jnp.concatenate([tok4[i, HEAD:] for i in range(PAIRS)], axis=1)
    den = jnp.concatenate([den_all[8 * i] for i in range(PAIRS)], axis=1)
    clip = jnp.maximum(den, 1.0)
    inverse = 1.0 / clip
    tokens = num * inverse
    maps = [a_ref[i] for i in range(3)]
    maps_t = jnp.concatenate([m.T for m in maps])
    qkv = dot(maps_t, tokens, precision=EXACT)
    q_t, k_t, v_t = qkv[:HEAD], qkv[HEAD : 2 * HEAD], qkv[2 * HEAD :]
    k_n, v_n = k_t.T, v_t.T
    scale = HEAD ** (-0.5)

    def on_diagonal(block):
        return jnp.concatenate([jnp.where(half, block, 0.0), jnp.where(half, 0.0, block)])

    mixed, grads = [], []
    for pair in range(PAIRS):
        cols = slice(pair * 2 * SLICES, (pair + 1) * 2 * SLICES)
        low = slice(pair * 2 * SLICES, pair * 2 * SLICES + SLICES)
        high = slice(pair * 2 * SLICES + SLICES, (pair + 1) * 2 * SLICES)
        q2, k2, v2, g2 = q_t[:, cols], k_t[:, cols], v_t[:, cols], g_mix[:, cols]
        scores = scale * jnp.where(
            half, dot(k_n[low], q2, precision=EXACT), dot(k_n[high], q2, precision=EXACT)
        )
        e = jnp.exp(scores - jnp.max(scores, axis=0, keepdims=True))
        attn = e * (1.0 / jnp.sum(e, axis=0, keepdims=True))
        attn2 = on_diagonal(attn)
        mixed.append(dot(v2, attn2, precision=EXACT))
        g_v = dot(g2, attn2, 1, 1, precision=EXACT)
        g_attn = jnp.where(
            half, dot(v_n[low], g2, precision=EXACT), dot(v_n[high], g2, precision=EXACT)
        )
        g_scores = attn * (g_attn - jnp.sum(g_attn * attn, axis=0, keepdims=True)) * scale
        g_scores2 = on_diagonal(g_scores)
        g_q = dot(k2, g_scores2, precision=EXACT)
        g_k = dot(q2, g_scores2, 1, 1, precision=EXACT)
        grads.append(jnp.concatenate([g_q, g_k, g_v]))
    mixed = jnp.concatenate(mixed, axis=1)
    grads = jnp.concatenate(grads, axis=1)
    g_tok = dot(jnp.concatenate(maps, axis=1), grads, precision=EXACT)
    g_num = g_tok * inverse
    g_den = jnp.where(
        den > 1.0, -jnp.sum(g_tok * tokens, axis=0, keepdims=True) * inverse, 0.0
    )

    mixed_half, num_half = mixed.astype(BF16), g_num.astype(BF16)
    table = jnp.concatenate([mixed_half, num_half])
    first = g_den.astype(BF16).astype(F32)
    second = (g_den - first).astype(BF16).astype(F32)
    third = g_den - first - second
    lines = jnp.concatenate(
        [
            table.astype(F32),
            first,
            second,
            third,
            jnp.zeros((2 * HEAD - 3, HEADS * SLICES), F32),
        ]
    )
    lines_t = lines.T.astype(BF16)
    ones = jnp.ones((2 * HEAD, points), BF16)
    row = lax.broadcasted_iota(jnp.int32, (HEAD, SLICES), 0)
    g_slice = jnp.zeros((HEAD, SLICES), F32)
    g_temp = jnp.zeros((HEAD, SLICES), F32)
    zero = jnp.zeros((), BF16)
    for pair in range(PAIRS):
        cols = slice(pair * 2 * SLICES, (pair + 1) * 2 * SLICES)
        w2 = wgt[pl.ds(pair * 2 * SLICES, 2 * SLICES), :]
        t2 = table[:, cols]
        back = dot(jnp.concatenate([jnp.where(half, t2, zero), jnp.where(half, zero, t2)]), w2)
        for i, h in enumerate((2 * pair, 2 * pair + 1)):
            rows = pl.ds(h * HEAD, HEAD)
            mrg[rows, :] = back[2 * HEAD * i : 2 * HEAD * i + HEAD].astype(BF16)
            xm = xmt[rows, :]
            right = jnp.concatenate([got[rows, :], xm, ones])
            g_w = dot(lines_t[h * SLICES : (h + 1) * SLICES], right)
            p = prob[pl.ds(h * SLICES, SLICES), :]
            g_logit = (p * live) * (g_w - jnp.sum(g_w * p, axis=0, keepdims=True))
            g_raw = (g_logit * rates[h]).astype(BF16)
            share = jnp.sum(
                jnp.sum(g_logit * logit[pl.ds(h * SLICES, SLICES), :], axis=0, keepdims=True)
                * rates[h],
                axis=1,
                keepdims=True,
            )
            g_temp = jnp.where(row == h, -share, g_temp)
            g_slice = g_slice + dot(xm, g_raw, 1, 1)
            total = back[2 * HEAD * i + HEAD : 2 * HEAD * (i + 1)] + dot(cluster, g_raw)
            gxm[rows, :] = total.astype(BF16)
    s_out[...] = jnp.concatenate([g_slice, g_temp], axis=1).reshape(PLANE, 1, 2 * SLICES)
    for i, grad in enumerate((dot(xt[...], gxm[...], 1, 1), dot(mrg[...], y_ref[...]))):
        grad = grad.astype(BF16)
        g_out[0, :, i] = grad[:, :128].reshape(16, 16, 128)
        g_out[1, :, i] = grad[:, 128:].reshape(16, 16, 128)

    def block_of(device):
        side = device // GRP
        return side // 4, lax.rem(device, GRP) * 4 + lax.rem(side, 4)

    def scatter_grads(r, carry):
        other, peer = plane_peer(r)
        col, block = block_of(other)
        push(g_out.at[col, block], g_in.at[r], 6, peer)
        push(s_out.at[other], s_in.at[r], 7, peer)
        return carry

    lax.fori_loop(1, PLANE, scatter_grads, 0)
    col, block = block_of(me)
    g_in[0] = g_out[col, block]
    s_in[0] = s_out[me]
    dx_ref[...] = dot(gxm[...], w_ref[...], 0, 1).astype(BF16)
    token_grads = dot(tokens, grads, 1, 1, precision=EXACT)
    for i in range(3):
        da_ref[i] = token_grads[:, i * HEAD : (i + 1) * HEAD]
    landed(g_in.at[pl.ds(1, PLANE - 1)], 6)
    landed(s_in.at[pl.ds(1, PLANE - 1)], 7)
    g_part[...] = jnp.sum(g_in[...].astype(F32), axis=0).astype(BF16)
    s_part[...] = jnp.sum(s_in[...], axis=0)

    def swap_grads(r, carry):
        push(g_part, g_z.at[z], 8, depth_peer(r))
        push(s_part, s_z.at[z], 9, depth_peer(r))
        return carry

    lax.fori_loop(1, depth, swap_grads, 0)
    g_z[z] = g_part[...]
    s_z[z] = s_part[...]
    landed(g_z.at[pl.ds(0, depth - 1)], 8)
    landed(s_z.at[pl.ds(0, depth - 1)], 9)
    g_sum[...] = jnp.sum(g_z[...].astype(F32), axis=0)
    s_sum[...] = jnp.sum(s_z[...], axis=0)

    def spread_grads(r, carry):
        push(g_sum, g_all.at[s], 10, side_peer(r))
        return carry

    def spread_small(r, carry):
        push(s_sum, s_all.at[me], 11, plane_peer(r)[1])
        return carry

    lax.fori_loop(1, SIDE, spread_grads, 0)
    lax.fori_loop(1, PLANE, spread_small, 0)
    g_all[s] = g_sum[...]
    s_all[me] = s_sum[...]
    landed(g_all.at[pl.ds(1, SIDE - 1)], 10)
    landed(s_all.at[pl.ds(1, PLANE - 1)], 11)
    for i in range(2):
        for side in range(SIDE):
            dw_ref[i, pl.ds(16 * (side % 4), 16), pl.ds(128 * (side // 4), 128)] = g_all[side, i]
    small = s_all[...].reshape(PLANE, 2 * SLICES)
    ds_ref[...] = small[:, :SLICES]
    at = lax.broadcasted_iota(jnp.int32, (HEADS, SLICES), 0)
    lane = lax.broadcasted_iota(jnp.int32, (HEADS, SLICES), 1)
    dt_ref[...] = jnp.sum(
        jnp.where(at == lane, small[:HEADS, SLICES:], 0.0), axis=0, keepdims=True
    )[:, :HEADS]

    left(tok_in.at[pl.ds(1, PLANE - 1)], 0)
    left(den_in.at[pl.ds(1, PLANE - 1)], 1)
    left(tok_z.at[pl.ds(0, depth - 1)], 2)
    left(den_z.at[pl.ds(0, depth - 1)], 3)
    left(tok_all.at[pl.ds(1, PLANE - 1)], 4)
    left(den_all.at[pl.ds(1, PLANE - 1)], 5)
    left(g_in.at[pl.ds(1, PLANE - 1)], 6)
    left(s_in.at[pl.ds(1, PLANE - 1)], 7)
    left(g_z.at[pl.ds(0, depth - 1)], 8)
    left(s_z.at[pl.ds(0, depth - 1)], 9)
    left(g_all.at[pl.ds(1, SIDE - 1)], 10)
    left(s_all.at[pl.ds(1, PLANE - 1)], 11)


def local(depth, x, y, w, e, c, t, a, tally):
    points, width = x.shape
    flat = HEADS * SLICES
    vmem = pl.BlockSpec(memory_space=pltpu.VMEM)
    smem = pl.BlockSpec(memory_space=pltpu.SMEM)
    lanes = 2 * SLICES
    dx, dw, ds, dt, da = pl.pallas_call(
        functools.partial(kernel, depth),
        name="layer",
        out_shape=(
            jax.ShapeDtypeStruct((points, width), BF16),
            jax.ShapeDtypeStruct((2, width // GRP, width), F32),
            jax.ShapeDtypeStruct((HEAD, SLICES), F32),
            jax.ShapeDtypeStruct((1, HEADS), F32),
            jax.ShapeDtypeStruct((3, HEAD, HEAD), F32),
        ),
        in_specs=[vmem, vmem, vmem, vmem, vmem, smem, vmem, smem],
        out_specs=[vmem] * 5,
        scratch_shapes=[
            pltpu.VMEM((width, points), BF16),
            pltpu.VMEM((width, points), BF16),
            pltpu.VMEM((flat, points), F32),
            pltpu.VMEM((flat, points), F32),
            pltpu.VMEM((flat, points), BF16),
            pltpu.VMEM((width, points), BF16),
            pltpu.VMEM((width, points), BF16),
            pltpu.VMEM((width, points), BF16),
            pltpu.VMEM((PLANE, 8, lanes), F32),
            pltpu.VMEM((PLANE, 1, lanes), F32),
            pltpu.VMEM((PLANE, 8, lanes), F32),
            pltpu.VMEM((PLANE, 1, lanes), F32),
            pltpu.VMEM((8, lanes), F32),
            pltpu.VMEM((1, lanes), F32),
            pltpu.VMEM((depth, 8, lanes), F32),
            pltpu.VMEM((depth, 1, lanes), F32),
            pltpu.VMEM((8, lanes), F32),
            pltpu.VMEM((1, lanes), F32),
            pltpu.VMEM((PLANE, 8, lanes), F32),
            pltpu.VMEM((PLANE, 1, lanes), F32),
            pltpu.VMEM((2, 16, 2, 16, 128), BF16),
            pltpu.VMEM((PLANE, 2, 16, 128), BF16),
            pltpu.VMEM((PLANE, 1, lanes), F32),
            pltpu.VMEM((PLANE, 1, lanes), F32),
            pltpu.VMEM((2, 16, 128), BF16),
            pltpu.VMEM((1, lanes), F32),
            pltpu.VMEM((depth, 2, 16, 128), BF16),
            pltpu.VMEM((depth, 1, lanes), F32),
            pltpu.VMEM((2, 16, 128), F32),
            pltpu.VMEM((1, lanes), F32),
            pltpu.VMEM((SIDE, 2, 16, 128), F32),
            pltpu.VMEM((PLANE, 1, lanes), F32),
            pltpu.SemaphoreType.DMA((12,)),
            pltpu.SemaphoreType.DMA((12,)),
        ],
        compiler_params=pltpu.CompilerParams(
            collective_id=0, has_side_effects=True, vmem_limit_bytes=40 * 1024 * 1024
        ),
    )(x, y, w, e, c, t, a, tally)
    return dx, dw, ds, dt.reshape(HEADS), da


def solution(mesh):
    depth = mesh.devices.size // PLANE
    finer = Mesh(mesh.devices.reshape(depth, SIDE, GRP), ("z", "s", "y"))
    rows = P(("z", "s", "y"), None)
    return jax.shard_map(
        functools.partial(local, depth),
        mesh=finer,
        in_specs=(rows, rows, P(), P(), P(), P(), P(), P()),
        out_specs=(rows, P(None, "y", None), P(), P(), P()),
        check_vma=False,
    )
```
